32 devices in a mesh: node: 8 (over z, y), feat: 4 (over x, core).
Axes of the slice: x: 2, y: 2, z: 4, core: 2. Of those that a mesh axis runs over, the one named last changes fastest.
Arguments:
- mesh_nodes: bfloat16 [2048, 512], P('node', 'feat'), may hold values from -6 to 6
- mesh_edges: bfloat16 [16384, 512], P(('node', 'feat')), may hold values from -6 to 6
- grid_nodes: bfloat16 [4096, 512], P('node', 'feat'), may hold values from -6 to 6
- m2g_edges: bfloat16 [12288, 512], P(('node', 'feat')), may hold values from -6 to 6
- edge_receivers: int32 [16384], P(('node', 'feat')), may hold values from 0 to 255
- edge_slots: int32 [16384], P(('node', 'feat')), may hold values from 0 to 1023
- send_rows: int32 [8, 8, 128], P('node'), may hold values from 0 to 255
- m2g_slots: int32 [12288], P(('node', 'feat')), may hold values from 0 to 1023
- m2g_send_rows: int32 [8, 8, 128], P('node'), may hold values from 0 to 255
- edge_w_in: bfloat16 [3, 3, 512, 512], replicated, may hold values from -0.15625 to 0.15625
- edge_w_out: bfloat16 [3, 512, 512], replicated, may hold values from -0.25 to 0.25
- edge_bias: float32 [3, 2, 512], replicated, may hold values from -2 to 2
- edge_gain: float32 [3, 512], replicated, may hold values from 0.5 to 1.5
- edge_shift: float32 [3, 512], replicated, may hold values from -2 to 2
- node_w_in: bfloat16 [3, 2, 512, 512], P(None, None, 'feat'), may hold values from -0.1875 to 0.1875
- node_w_out: bfloat16 [3, 512, 512], P(None, 'feat'), may hold values from -0.25 to 0.25
- node_bias: float32 [3, 2, 512], P(None, None, 'feat'), may hold values from -2 to 2
- node_gain: float32 [3, 512], P(None, 'feat'), may hold values from 0.5 to 1.5
- node_shift: float32 [3, 512], P(None, 'feat'), may hold values from -2 to 2
Outputs:
- grid_out: bfloat16 [4096, 512], P('node', 'feat')
The draws below stay inside these ranges and needn't reach their ends.
All inputs are finite; a program needn't handle non-finite values.
Results may differ from the reference program's by a relative error of at most 0.015.
Values may be sent and summed in bfloat16 or wider, within the bound.
A program may use at most 64 MiB of HBM per device.

```python
import jax
import jax.numpy as jnp
from jax import lax

D = 512
NODE_DEV = 256
GRID_DEV = 512
LAYERS = 2
EDGE_DEV = 2048
M2G_DEV = 1536
BLOCK_BUF = 1024
SLOT = 128
M2G_BUF = 1024
M2G_SLOT = 128
NODES = 2048
EDGES = 16384
GRIDS = 4096
M2G_EDGES = 12288
N_NODE = 8


def touch_ends(drawn, stream_key, low, high):
    longest = drawn.shape.index(max(drawn.shape))
    spots = []
    for shift in (0, 1):
        where = [jax.random.randint(jax.random.fold_in(stream_key, axis), (), 0, length) for axis, length in enumerate(drawn.shape)]
        where[longest] = (where[longest] + shift) % drawn.shape[longest]
        spots.append(tuple(where))
    return drawn.at[spots[0]].set(low).at[spots[1]].set(high)


def block_levels(stream_key, extent, split, smallest, top_value):
    def one(dim, parts):
        steps = jax.random.uniform(jax.random.fold_in(jax.random.fold_in(stream_key, 6), dim), (parts,), jnp.float32, smallest / len(split), top_value / len(split))
        return jnp.repeat(jnp.exp(steps), extent[dim] // parts).reshape((-1,) + (1,) * (len(extent) - dim - 1))

    level = one(*split[0])
    for cut in split[1:]:
        level = level * one(*cut)
    return level


def centred(own_key, dims, scale, limit, shards=(), held_as=jnp.bfloat16):
    result = scale * jax.random.normal(own_key, dims, jnp.float32)
    if shards:
        result = result * block_levels(own_key, dims, shards, -0.22, 0.18)
    return jnp.clip(result, -limit, limit).astype(held_as)


def setup_inputs(seed: int = 0) -> dict:
    splits = jax.random.split(jax.random.key(seed), 20)
    return {
        "mesh_nodes": centred(splits[0], (NODES, D), 1.0, 6.0, ((0, 8), (1, 4))),
        "mesh_edges": centred(splits[1], (EDGES, D), 1.0, 6.0, ((0, 32),)),
        "grid_nodes": centred(splits[2], (GRIDS, D), 1.0, 6.0, ((0, 8), (1, 4))),
        "m2g_edges": centred(splits[3], (M2G_EDGES, D), 1.0, 6.0, ((0, 32),)),
        "edge_receivers": touch_ends(jax.random.randint(splits[4], (EDGES,), 0, NODE_DEV), jax.random.fold_in(splits[4], 1), 0, NODE_DEV - 1).astype(jnp.int32),
        "edge_slots": touch_ends(jax.random.randint(splits[5], (EDGES,), 0, BLOCK_BUF), jax.random.fold_in(splits[5], 1), 0, BLOCK_BUF - 1).astype(jnp.int32),
        "send_rows": touch_ends(jax.random.randint(splits[6], (N_NODE, N_NODE, SLOT), 0, NODE_DEV), jax.random.fold_in(splits[6], 1), 0, NODE_DEV - 1).astype(jnp.int32),
        "m2g_slots": touch_ends(jax.random.randint(splits[7], (M2G_EDGES,), 0, M2G_BUF), jax.random.fold_in(splits[7], 1), 0, M2G_BUF - 1).astype(jnp.int32),
        "m2g_send_rows": touch_ends(jax.random.randint(splits[8], (N_NODE, N_NODE, M2G_SLOT), 0, NODE_DEV), jax.random.fold_in(splits[8], 1), 0, NODE_DEV - 1).astype(jnp.int32),
        "edge_w_in": centred(splits[9], (LAYERS + 1, 3, D, D), (3 * D) ** -0.5, 0.15625),
        "edge_w_out": centred(splits[10], (LAYERS + 1, D, D), D ** -0.5, 0.25),
        "edge_bias": centred(splits[11], (LAYERS + 1, 2, D), 0.3, 2.0, (), jnp.float32),
        "edge_gain": jnp.clip(1.0 + 0.1 * jax.random.normal(splits[12], (LAYERS + 1, D), jnp.float32), 0.5, 1.5),
        "edge_shift": centred(splits[13], (LAYERS + 1, D), 0.3, 2.0, (), jnp.float32),
        "node_w_in": centred(splits[14], (LAYERS + 1, 2, D, D), (2 * D) ** -0.5, 0.1875, ((2, 4),)),
        "node_w_out": centred(splits[15], (LAYERS + 1, D, D), D ** -0.5, 0.25, ((1, 4),)),
        "node_bias": centred(splits[16], (LAYERS + 1, 2, D), 0.3, 2.0, ((2, 4),), jnp.float32),
        "node_gain": jnp.clip(1.0 + 0.1 * jax.random.normal(splits[17], (LAYERS + 1, D), jnp.float32), 0.5, 1.5),
        "node_shift": centred(splits[18], (LAYERS + 1, D), 0.3, 2.0, ((1, 4),), jnp.float32),
    }


EPSILON = 1e-05

def perceptron(inputs, weight_in, weight_out, bias_pair, gain_row, shift_row):
    hidden_pre = jnp.zeros((inputs[0].shape[0], weight_out.shape[1]), jnp.float32) + bias_pair[0].astype(jnp.float32)
    for term_index in range(len(inputs)):
        hidden_pre = hidden_pre + jnp.dot(inputs[term_index], weight_in[term_index], preferred_element_type=jnp.float32)
    hidden = jax.nn.silu(hidden_pre).astype(jnp.bfloat16)
    projected = jnp.dot(hidden, weight_out, preferred_element_type=jnp.float32) + bias_pair[1].astype(jnp.float32)
    mean_row = lax.optimization_barrier(jnp.mean(projected, axis=-1, keepdims=True))
    variance = lax.optimization_barrier(jnp.mean(projected * projected, axis=-1, keepdims=True)) - mean_row * mean_row
    normed = (projected - mean_row) * lax.rsqrt(variance + EPSILON) * gain_row + shift_row
    return (inputs[0].astype(jnp.float32) + normed).astype(jnp.bfloat16)

def reference(mesh_nodes, mesh_edges, grid_nodes, m2g_edges, edge_receivers, edge_slots, send_rows, m2g_slots, m2g_send_rows, edge_w_in, edge_w_out, edge_bias, edge_gain, edge_shift, node_w_in, node_w_out, node_bias, node_gain, node_shift):
    blocks = jnp.arange(N_NODE, dtype=jnp.int32)
    latent = mesh_nodes
    edge_latent = mesh_edges
    for layer_index in range(LAYERS):

        def edge_block(packed, latent=latent, layer_index=layer_index):
            block, block_edges, block_receivers, block_slots = packed
            source = (block_slots // SLOT).astype(jnp.int32)
            chosen = send_rows[source, block, block_slots % SLOT]
            senders = latent[source * NODE_DEV + chosen]
            receivers = latent[block * NODE_DEV + block_receivers]
            updated = perceptron((block_edges, senders, receivers), edge_w_in[layer_index], edge_w_out[layer_index], edge_bias[layer_index], edge_gain[layer_index], edge_shift[layer_index])
            summed = jax.ops.segment_sum(updated.astype(jnp.float32), block_receivers, num_segments=NODE_DEV)
            return (updated, summed.astype(jnp.bfloat16))
        edge_latent, summed = lax.map(edge_block, (blocks, edge_latent.reshape(N_NODE, EDGE_DEV, D), edge_receivers.reshape(N_NODE, EDGE_DEV), edge_slots.reshape(N_NODE, EDGE_DEV)))
        edge_latent = edge_latent.reshape(EDGES, D)
        summed = summed.reshape(NODES, D)
        latent = perceptron((latent, summed), node_w_in[layer_index], node_w_out[layer_index], node_bias[layer_index], node_gain[layer_index], node_shift[layer_index])

    def link_block(packed):
        block, block_links, block_cells, block_slots = packed
        source = (block_slots // M2G_SLOT).astype(jnp.int32)
        chosen = m2g_send_rows[source, block, block_slots % M2G_SLOT]
        senders = latent[source * NODE_DEV + chosen]
        receivers = jnp.broadcast_to(block_cells[:, None, :], (GRID_DEV, 3, D)).reshape(M2G_DEV, D)
        updated = perceptron((block_links, senders, receivers), edge_w_in[LAYERS], edge_w_out[LAYERS], edge_bias[LAYERS], edge_gain[LAYERS], edge_shift[LAYERS])
        return updated.astype(jnp.float32).reshape(GRID_DEV, 3, D).sum(axis=1).astype(jnp.bfloat16)
    grid_summed = lax.map(link_block, (blocks, m2g_edges.reshape(N_NODE, M2G_DEV, D), grid_nodes.reshape(N_NODE, GRID_DEV, D), m2g_slots.reshape(N_NODE, M2G_DEV)))
    grid_summed = grid_summed.reshape(GRIDS, D)
    return perceptron((grid_nodes, grid_summed), node_w_in[LAYERS], node_w_out[LAYERS], node_bias[LAYERS], node_gain[LAYERS], node_shift[LAYERS])
```

```python
import functools

import jax
import jax.numpy as jnp
from jax import lax
from jax.experimental import pallas as pl
from jax.experimental.pallas import tpu as pltpu
from jax.sharding import PartitionSpec as P

EPSILON = 1e-05
LANES = 128
BF16 = jnp.bfloat16
F32 = jnp.float32
MESH = pl.DeviceIdType.MESH


def dot(a, b):
    return jnp.dot(a, b, preferred_element_type=F32)


def at(start, size):
    return pl.ds(pl.multiple_of(start * size, size), size)


def column(row):
    return jnp.transpose(jnp.broadcast_to(row, (LANES, row.shape[1])))


def fill_picks(ref, row):
    col = column(row)
    lane = lax.broadcasted_iota(jnp.int32, col.shape, 1)
    for c in range(0, ref.shape[1], LANES):
        ref[:, c : c + LANES] = jnp.where(col == lane + c, 1.0, 0.0).astype(BF16)


def finish_mlp(pre, base, w_out, bias_out, gain, shift):
    h = 0.5 * pre
    hidden = (h + h * jnp.tanh(h)).astype(BF16)
    out = dot(hidden, w_out) + bias_out
    mean = jnp.mean(out, axis=-1, keepdims=True)
    variance = jnp.mean(out * out, axis=-1, keepdims=True) - mean * mean
    normed = (out - mean) * lax.rsqrt(variance + EPSILON) * gain + shift
    return (base.astype(F32) + normed).astype(BF16)


def kernel(n, feats, counts, *refs):
    (
        nodes, edges_hbm, grid_hbm, links_hbm, recv_row, slot_row, table_row, link_row, link_table_row,
        ew_in_hbm, ew_out_hbm, ebias, egain, eshift, nw_in_hbm, nw_out_hbm, nbias, ngain, nshift,
        out,
        edges, links, ew_in, ew_out, nw_in, nw_out, nb, ng, ns,
        pick_table, pick_link_table, pick_slot, pick_recv, sum_recv, pick_link, pick_cell, sum_cell,
        acc, part, chip_sum, rs_buf, cells, upd, wide, outgoing, extra, arrived, latent_pre,
        load_sem, send_sem, recv_sem,
    ) = refs
    sections = ew_in.shape[0]
    last = sections - 1
    p = lax.axis_index("node")
    f = lax.axis_index("feat")
    half = feats // 2
    chip = lax.div(f, 2)
    core = lax.rem(f, 2)
    partner = f + 1 - 2 * core
    role = lax.rem(p, 2)
    beside = p + 1 - 2 * role
    block_half = n // 2
    rows_all, share = nodes.shape
    own_rows = rows_all // 2
    cell_count = cells.shape[0]
    next_sem = [0]

    def sems(count):
        base = next_sem[0]
        next_sem[0] += count
        return base

    def remote(src, dst, sem, **where):
        return pltpu.make_async_remote_copy(
            src_ref=src, dst_ref=dst, send_sem=send_sem.at[sem], recv_sem=recv_sem.at[sem],
            device_id=where, device_id_type=MESH,
        )

    def peer(k):
        out, bit = p, 1
        while bit < n:
            if isinstance(k, int):
                if k & bit:
                    out = out + bit * (1 - 2 * lax.rem(lax.div(p, bit), 2))
            else:
                ours, theirs = lax.rem(lax.div(p, bit), 2), lax.rem(lax.div(k, bit), 2)
                out = out + bit * (lax.rem(ours + theirs, 2) - ours)
            bit *= 2
        return out

    def feat_at(k):
        return lax.rem(f + k, feats)

    def chip_at(m):
        return lax.rem(chip + m, half) * 2 + core

    def chip_from(m):
        return lax.rem(chip + half - m, half) * 2 + core

    barrier = pltpu.get_barrier_semaphore()

    def greet(k, carry):
        pl.semaphore_signal(barrier, inc=1, device_id={"node": peer(k)}, device_id_type=MESH)
        return carry

    lax.fori_loop(1, n, greet, 0)
    for k in range(1, feats):
        pl.semaphore_signal(barrier, inc=1, device_id={"feat": feat_at(k)}, device_id_type=MESH)

    loads = {}

    def load(name, src, dst):
        copy = pltpu.make_async_copy(src, dst, load_sem.at[len(loads)])
        copy.start()
        loads[name] = copy

    load("wide", nodes, wide.at[0, :, at(f, share)])
    load("edges", edges_hbm, edges)
    for t in range(sections):
        load(("ew_in", t), ew_in_hbm.at[t], ew_in.at[t])
        load(("ew_out", t), ew_out_hbm.at[t], ew_out.at[t])
        load(("nw_in", t), nw_in_hbm.at[t], nw_in.at[t, :, at(f, share), :])
        load(("nw_out", t), nw_out_hbm.at[t], nw_out.at[t, at(f, share), :])
    load("links", links_hbm, links)
    load("cells", grid_hbm.at[at(f, cell_count), :], cells.at[:, at(f, share)])
    load("nb", nbias, nb.at[f])
    load("ng", ngain, ng.at[f])
    load("ns", nshift, ns.at[f])

    pick_refs = [pick_table] * last + [pick_link_table]
    slots = [c // n for c in counts]
    groups = [min(2 * LANES // s, n // 2) for s in slots]

    fill_picks(pick_table, table_row[...])
    first_out = dot(pick_table[...], nodes[...]).astype(BF16)
    outgoing[0, : counts[0], :] = first_out

    pl.semaphore_wait(barrier, n - 1 + feats - 1)

    node_sem = [sems(n) for _ in range(sections)]
    near_sem = [sems(n) for _ in range(sections)]
    chips = range(1, half)
    swap_sem = [{m: sems(n) for m in chips} for _ in range(sections)]
    relay_sem = [{m: sems(n) for m in chips} for _ in range(sections)]

    def each(fn, ks):
        if len(ks) <= 8:
            for k in ks:
                fn(k)
        else:

            def body(i, carry):
                fn(ks.start + i * ks.step)
                return carry

            lax.fori_loop(0, len(ks), body, 0)

    far = range(n - 1, n // 2 - 1, -1)
    close = range(1, n // 2)

    def node_copy(t, k):
        dst = peer(k)
        return remote(
            outgoing.at[t, at(dst, slots[t]), :],
            arrived.at[t, at(p, slots[t]), at(f, share)],
            node_sem[t] + k, node=dst,
        )

    def block(t, k, who):
        return arrived.at[t, at(peer(k), slots[t]), at(who, share)]

    def near_copy(t, k):
        return remote(block(t, k, f), block(t, k, f), near_sem[t] + k, feat=partner)

    def far_copy(t, k, m):
        return remote(block(t, k, f), block(t, k, f), swap_sem[t][m] + k, feat=chip_at(m))

    def extra_copy(t, k, m):
        dst = peer(k)
        return remote(
            extra.at[t, m, at(dst, slots[t]), :],
            arrived.at[t, at(p, slots[t]), at(chip_from(m), share)],
            swap_sem[t][m] + k, node=dst,
        )

    def relay_copy(t, k, m):
        who = chip_from(m)
        return remote(block(t, k, who), block(t, k, who), relay_sem[t][m] + k, feat=partner)

    def take_far(t, k):
        node_copy(t, k).wait_recv()
        for m in chips:
            far_copy(t, k, m).start()
        near_copy(t, k).start()

    def take_close(t, k):
        node_copy(t, k).wait_recv()
        near_copy(t, k).start()

    def relay_far(t, k):
        for m in chips:
            far_copy(t, k, m).wait_recv()
            relay_copy(t, k, m).start()

    def relay_close(t, k):
        for m in chips:
            extra_copy(t, k, m).wait_recv()
            relay_copy(t, k, m).start()

    def arrive(t, k):
        near_copy(t, k).wait_recv()
        for m in chips:
            relay_copy(t, k, m).wait_recv()

    def settle(t):
        def sent(k):
            node_copy(t, k).wait_send()
            near_copy(t, k).wait_send()
            for m in chips:
                relay_copy(t, k, m).wait_send()

        def far_sent(k):
            for m in chips:
                far_copy(t, k, m).wait_send()

        def close_sent(k):
            for m in chips:
                extra_copy(t, k, m).wait_send()

        each(sent, range(1, n))
        each(far_sent, far)
        each(close_sent, close)

    def weight_copies(near_src, near_dst, half_src, half_dst):
        group = {"near": [remote(near_src, near_dst, sems(1), feat=partner)]}
        for name in ("far", "back", "side", "last"):
            group[name] = []
        for m in chips:
            who = chip_from(m)
            group["far"].append(remote(half_src, half_dst(f, role), sems(1), feat=chip_at(m)))
            group["back"].append(remote(half_dst(who, role), half_dst(who, role), sems(1), feat=partner))
            group["side"].append(remote(half_dst(who, role), half_dst(who, role), sems(1), node=beside))
            other = half_dst(who, 1 - role)
            group["last"].append(remote(other, other, sems(1), feat=partner))
        return group

    half_share = share // 2

    def out_rows(who, part_id):
        return at(who * 2 + part_id, half_share)

    weights_in = [
        weight_copies(
            nw_in_hbm.at[t], nw_in.at[t, :, at(f, share), :], nw_in_hbm.at[t, role],
            lambda who, part_id, t=t: nw_in.at[t, part_id, at(who, share), :],
        )
        for t in range(sections)
    ]
    weights_out = [
        weight_copies(
            nw_out_hbm.at[t], nw_out.at[t, at(f, share), :], nw_out_hbm.at[t, at(role, half_share), :],
            lambda who, part_id, t=t: nw_out.at[t, out_rows(who, part_id), :],
        )
        for t in range(sections)
    ]

    def begin(group):
        for copy in group["far"] + group["near"]:
            copy.start()

    def pass_on(group):
        for far, back, side in zip(group["far"], group["back"], group["side"]):
            far.wait_recv()
            side.start()
            back.start()

    def pass_last(group):
        for side, copy in zip(group["side"], group["last"]):
            side.wait_recv()
            copy.start()

    def complete(group):
        for copy in group["near"] + group["back"] + group["last"]:
            copy.wait()
        for copy in group["far"] + group["side"]:
            copy.wait_send()

    def over_feat(make):
        base = sems(feats)
        return [make(k, base + k, feat_at(k)) for k in range(1, feats)]

    each(lambda k: node_copy(0, k).start(), far)
    each(lambda k: node_copy(0, k).start(), close)

    def wide_cols(who):
        return wide.at[0, :, at(who, share)]

    wide_near = remote(nodes, wide_cols(f), sems(1), feat=partner)
    wide_far = [remote(nodes, wide_cols(f), sems(1), feat=chip_at(m)) for m in chips]
    wide_back = [remote(wide_cols(chip_from(m)), wide_cols(chip_from(m)), sems(1), feat=partner) for m in chips]
    for copy in wide_far + [wide_near]:
        copy.start()
    begin(weights_in[0])
    begin(weights_out[0])
    small = []
    for src, dst in ((nbias, nb), (ngain, ng), (nshift, ns)):
        small += over_feat(lambda k, sem, who, src=src, dst=dst: remote(src, dst.at[f], sem, feat=who))
    cell_copies = over_feat(
        lambda k, sem, dst: remote(grid_hbm.at[at(dst, cell_count), :], cells.at[:, at(f, share)], sem, feat=dst)
    )
    for copy in small:
        copy.start()

    fill_picks(pick_slot, slot_row[...])
    fill_picks(pick_recv, recv_row[...])
    node_id = lax.broadcasted_iota(jnp.int32, sum_recv.shape, 0)
    sum_recv[...] = jnp.where(node_id == recv_row[...], 1.0, 0.0).astype(BF16)
    fill_picks(pick_link, link_row[...].reshape(1, -1))
    fill_picks(pick_link_table, link_table_row[...])
    link_id = lax.broadcasted_iota(jnp.int32, pick_cell.shape, 0)
    cell_id = 3 * lax.broadcasted_iota(jnp.int32, pick_cell.shape, 1)
    pick_cell[...] = jnp.where((link_id >= cell_id) & (link_id < cell_id + 3), 1.0, 0.0).astype(BF16)
    link_id = lax.broadcasted_iota(jnp.int32, sum_cell.shape, 1)
    cell_id = 3 * lax.broadcasted_iota(jnp.int32, sum_cell.shape, 0)
    sum_cell[...] = jnp.where((link_id >= cell_id) & (link_id < cell_id + 3), 1.0, 0.0).astype(BF16)

    def halves(count):
        tile = count // 2
        return [slice(i * tile, (i + 1) * tile) for i in range(2)]

    def edge_base(t, state, picks, source):
        loads[("ew_in", t)].wait()
        loads[("ew_out", t)].wait()
        got = dot(source[...], ew_in[t, 2]).astype(BF16)
        for rows in halves(state.shape[0]):
            acc[rows, :] = dot(state[rows, :], ew_in[t, 0]) + dot(picks[rows, :], got) + ebias[t, 0:1, :]

    def group_of(t, j):
        group = groups[t]
        rows = at(lax.div(peer(j * group), group), group * slots[t])
        return rows, dot(arrived[t, rows, :], ew_in[t, 1]).astype(BF16)

    def group_ks(t, j):
        return range(max(1, j * groups[t]), (j + 1) * groups[t])

    def edge_group(t, state, picks, j):
        each(lambda k: arrive(t, k), group_ks(t, j))
        cols, got = group_of(t, j)
        for rows in halves(state.shape[0]):
            acc[rows, :] += dot(picks[rows, cols], got)

    def edge_finish(t, state, picks, j):
        each(lambda k: arrive(t, k), group_ks(t, j))
        cols, got = group_of(t, j)
        for rows in halves(state.shape[0]):
            pre = acc[rows, :] + dot(picks[rows, cols], got)
            state[rows, :] = finish_mlp(
                pre, state[rows, :], ew_out[t], ebias[t, 1:2, :], egain[t : t + 1, :], eshift[t : t + 1, :]
            )

    def row(ref, t, *index):
        return jnp.concatenate([ref[(g, t) + index] for g in range(feats)], axis=-1).reshape(1, -1)

    def node_start(t, latent):
        latent_pre[: latent.shape[0], :] = dot(latent, nw_in[t, 0]) + row(nb, t, 0)

    def node_finish(t, latent, summed):
        pre = dot(summed, nw_in[t, 1]) + latent_pre[: latent.shape[0], :]
        return finish_mlp(pre, latent, nw_out[t], row(nb, t, 1), row(ng, t), row(ns, t))

    def weights_done(t):
        pass_last(weights_in[t])
        pass_last(weights_out[t])

    def weights_ready(t):
        loads[("nw_in", t)].wait()
        loads[("nw_out", t)].wait()
        complete(weights_in[t])
        complete(weights_out[t])

    mine = at(core, own_rows)
    for t in range(sections):
        state = links if t == last else edges
        picks = pick_link if t == last else pick_slot
        count = n // groups[t]
        far_groups = list(range(count - 1, count // 2 - 1, -1))
        if t == 0:
            loads["edges"].wait()
            loads["wide"].wait()
            for copy, back in zip(wide_far, wide_back):
                copy.wait_recv()
                back.start()
            for copy in [wide_near] + wide_back:
                copy.wait_recv()
        else:
            outgoing[t, : counts[t], :] = dot(pick_refs[t][...], wide[t, :, at(f, share)]).astype(BF16)
            each(lambda k, t=t: node_copy(t, k).start(), far)
            each(lambda k, t=t: node_copy(t, k).start(), close)
            if t == last:
                loads["links"].wait()
        for m in chips:
            cols = wide[t, :, at(chip_from(m), share)]
            extra[t, m, : counts[t], :] = dot(pick_refs[t][...], cols).astype(BF16)

        def extra_start(k, t=t):
            for m in chips:
                extra_copy(t, k, m).start()

        each(extra_start, close)
        own_slots = at(p, slots[t])
        arrived[t, own_slots, :] = dot(pick_refs[t][own_slots, :], wide[t]).astype(BF16)
        if t == last:
            loads["cells"].wait()
            for copy in cell_copies:
                copy.wait()
            edge_base(t, state, pick_cell, cells)
        else:
            edge_base(t, state, pick_recv, wide.at[t])
        for i, j in enumerate(far_groups):
            each(lambda k, t=t: take_far(t, k), group_ks(t, j)[::-1])
            if i == 0:
                if t > 0:
                    pass_on(weights_in[t])
                    pass_on(weights_out[t])
                each(lambda k, t=t: take_close(t, k), close)
                each(lambda k, t=t: relay_close(t, k), close)
        if t == 0:
            pass_on(weights_in[t])
            pass_on(weights_out[t])
        for i, j in enumerate(far_groups):
            if t > 0 and i == len(far_groups) - 1:
                weights_done(t)
            each(lambda k, t=t: relay_far(t, k), group_ks(t, j)[::-1])
            if i == 0:
                for c in range(count // 2):
                    edge_group(t, state, picks, c)
            else:
                edge_group(t, state, picks, far_groups[i - 1])
        if t == last:
            weights_ready(t)
            node_start(t, cells[...])
        edge_finish(t, state, picks, far_groups[-1])
        if t < last:
            part[t] = dot(sum_recv[at(1 - core, own_rows), :], edges[...]).astype(BF16)
            pair = remote(part.at[t], rs_buf.at[t, 0], sems(1), feat=partner)
            pair.start()
            total = dot(sum_recv[mine, :], edges[...])
            pair.wait()
            chip_sum[t] = (total + rs_buf[t, 0].astype(F32)).astype(BF16)
            sum_copies = [remote(chip_sum.at[t], rs_buf.at[t, m], sems(1), feat=chip_at(m)) for m in chips]
            for copy in sum_copies:
                copy.start()
            if t == 0:
                for copy in cell_copies:
                    copy.start()
                weights_done(t)
                for copy in [wide_near] + wide_far + wide_back:
                    copy.wait_send()
                for name in ("nb", "ng", "ns"):
                    loads[name].wait()
                for copy in small:
                    copy.wait()
            settle(t)
            weights_ready(t)
            node_start(t, wide[t, mine, :])
            summed = chip_sum[t].astype(F32)
            for m, copy in zip(chips, sum_copies):
                copy.wait()
                summed += rs_buf[t, m].astype(F32)
            begin(weights_in[t + 1])
            begin(weights_out[t + 1])
            wide[t + 1, mine, :] = node_finish(t, wide[t, mine, :], summed.astype(BF16))
            row_copy = remote(wide.at[t + 1, mine, :], wide.at[t + 1, mine, :], sems(1), feat=partner)
            row_copy.start()
            row_copy.wait()
    gathered = dot(sum_cell[...], links[...]).astype(BF16)
    upd[...] = node_finish(last, cells[...], gathered)
    out_copies = over_feat(
        lambda k, sem, dst: remote(upd.at[:, at(dst, share)], out.at[at(f, cell_count), :], sem, feat=dst)
    )
    for copy in out_copies:
        copy.start()
    out[at(f, cell_count), :] = upd[:, at(f, share)]
    settle(last)
    for copy in out_copies:
        copy.wait()
    assert next_sem[0] <= send_sem.shape[0]


def solution(mesh):
    n, feats = mesh.shape["node"], mesh.shape["feat"]

    def local(
        mesh_nodes, mesh_edges, grid_nodes, m2g_edges, edge_receivers, edge_slots, send_rows, m2g_slots,
        m2g_send_rows, edge_w_in, edge_w_out, edge_bias, edge_gain, edge_shift, node_w_in, node_w_out,
        node_bias, node_gain, node_shift,
    ):
        rows, share = mesh_nodes.shape
        edge_count, width = mesh_edges.shape
        link_count = m2g_edges.shape[0]
        sections = edge_w_in.shape[0]
        buf, link_buf = send_rows.size, m2g_send_rows.size
        cell_count = grid_nodes.shape[0] // feats
        counts = (buf,) * (sections - 1) + (link_buf,)
        top = max(counts)
        half = feats // 2
        sem_count = sections * n * (2 + 3 * (half - 1)) + 2 * sections * (1 + 4 * half) + feats * 6 + sections * feats + 2 * half
        vmem = pl.BlockSpec(memory_space=pltpu.VMEM)
        hbm = pl.BlockSpec(memory_space=pl.ANY)

        def v(*shape, dtype=BF16):
            return pltpu.VMEM(shape, dtype)

        return pl.pallas_call(
            functools.partial(kernel, n, feats, counts),
            name="graph_layers",
            out_shape=jax.ShapeDtypeStruct(grid_nodes.shape, BF16),
            in_specs=[
                vmem, hbm, hbm, hbm, vmem, vmem, vmem, vmem, vmem,
                hbm, hbm, vmem, vmem, vmem, hbm, hbm, vmem, vmem, vmem,
            ],
            out_specs=vmem,
            scratch_shapes=[
                v(edge_count, width), v(link_count, width),
                v(*edge_w_in.shape), v(*edge_w_out.shape),
                v(sections, 2, width, width), v(sections, width, width),
                v(feats, *node_bias.shape, dtype=F32), v(feats, *node_gain.shape, dtype=F32),
                v(feats, *node_shift.shape, dtype=F32),
                v(buf, rows), v(link_buf, rows), v(edge_count, buf), v(edge_count, rows), v(rows, edge_count),
                v(link_count, link_buf), v(link_count, cell_count), v(cell_count, link_count),
                v(max(edge_count, link_count), width, dtype=F32),
                v(sections - 1, rows // 2, width), v(sections - 1, rows // 2, width),
                v(sections - 1, half, rows // 2, width),
                v(cell_count, width), v(cell_count, width),
                v(sections, rows, width), v(sections, top, share), v(sections, half, top, share),
                v(sections, top, width), v(max(rows // 2, cell_count), width, dtype=F32),
                pltpu.SemaphoreType.DMA((7 + 4 * sections,)),
                pltpu.SemaphoreType.DMA((sem_count,)),
                pltpu.SemaphoreType.DMA((sem_count,)),
            ],
            compiler_params=pltpu.CompilerParams(
                collective_id=0, has_side_effects=True, vmem_limit_bytes=56 * 1024 * 1024
            ),
        )(
            mesh_nodes, mesh_edges, grid_nodes, m2g_edges, edge_receivers.reshape(1, -1), edge_slots.reshape(1, -1),
            send_rows.reshape(1, -1), m2g_slots, m2g_send_rows.reshape(1, -1),
            edge_w_in, edge_w_out, edge_bias, edge_gain, edge_shift, node_w_in, node_w_out,
            node_bias, node_gain, node_shift,
        )

    in_specs = (
        P("node", "feat"), P(("node", "feat"), None), P("node", "feat"), P(("node", "feat"), None),
        P(("node", "feat")), P(("node", "feat")), P("node", None, None), P(("node", "feat")),
        P("node", None, None), P(), P(), P(), P(), P(), P(None, None, "feat", None),
        P(None, "feat", None), P(None, None, "feat"), P(None, "feat"), P(None, "feat"),
    )
    return jax.shard_map(local, mesh=mesh, in_specs=in_specs, out_specs=P("node", "feat"), check_vma=False)
```
